32 devices in a mesh: grp: 8 (over y, x, core), mem: 4 (over z).
Axes of the slice: x: 2, y: 2, z: 4, core: 2. Of those that a mesh axis runs over, the one named last changes fastest.
Arguments:
- inverse: bfloat16 [64, 2048, 2048], P(('grp', 'mem')), may hold values from -0.125 to 0.125
- sources: bfloat16 [64, 2048, 256], P(('grp', 'mem')), may hold values from -6 to 6
- slot_blocks: int32 [32, 20], P(('grp', 'mem')), may hold values from -1 to 31, as said below
Outputs:
- controls: float32 [32, 20, 32768], P(('grp', 'mem'))
- states: bfloat16 [64, 2048, 256], P(('grp', 'mem'))
The draws below stay inside these ranges and needn't reach their ends.
Inputs may be any that keep to these rules, and one draw needn't show every extreme that they name: `slot_blocks`: slots pair up: slot s of a device and the slot named its partner are both empty or both filled. Toward each neighbouring cluster a device fills its first slots, from 1 to 6 of them; toward each other device of its cluster its first 1 to 2 slots; toward itself none. 6 and 2 are reached in every draw. Several slots may name one position.
All inputs are finite; a program needn't handle non-finite values.
Results may differ from the reference program's by a relative error of at most 0.004.
Values may be sent and summed in bfloat16 or wider, within the bound.
A program may use at most 128 MiB of HBM per device.

```python
import jax
import jax.numpy as jnp
from jax import lax

M = 2048
BLOCK = 128
R = 256
F_DEV = 2
CAP = 6
CAPM = 2
ITERS = 2
NB = 32
GROUPS = 8
MEMBERS = 4
DEVS = 32
FRACS = 64
N_GRP = 8
N_MEM = 4


def draw_slot_blocks(key, part):
    keys = jax.random.split(jax.random.fold_in(key, 17), 3)
    links = jax.random.randint(keys[0], (GROUPS, MEMBERS), 1, CAP + 1)
    links = links.at[0, 0].set(CAP)
    paired = jax.random.randint(keys[1], (GROUPS, MEMBERS, MEMBERS), 1, CAPM + 1)
    paired = jnp.minimum(paired, jnp.swapaxes(paired, 1, 2))
    paired = paired.at[0, 0, 1].set(CAPM).at[0, 1, 0].set(CAPM)
    same = jnp.arange(MEMBERS)[:, None] == jnp.arange(MEMBERS)[None, :]
    paired = jnp.where(same[None, :, :], 0, paired)
    slot = jnp.arange(CAP)
    ahead_live = slot[None, None, :] < links[:, :, None]
    behind_live = slot[None, None, :] < jnp.roll(links, 1, axis=0)[:, :, None]
    cross_live = jnp.arange(CAPM)[None, None, None, :] < paired[:, :, :, None]
    live = jnp.concatenate([ahead_live, behind_live, cross_live.reshape(GROUPS, MEMBERS, MEMBERS * CAPM)], axis=2)
    chosen = jax.random.randint(keys[2], (GROUPS, MEMBERS, 2 * CAP + MEMBERS * CAPM), 0, NB)
    return jnp.where(live, chosen, -1).reshape(DEVS, 2 * CAP + MEMBERS * CAPM).astype(jnp.int32)


def block_levels(key, shape, cuts, smallest, largest):
    loudness, own = 1.0, jax.random.fold_in(key, 6)
    for dim, shards_of in cuts:
        draws = jnp.exp(jax.random.uniform(jax.random.fold_in(own, dim), (shards_of,), jnp.float32, smallest / len(cuts), largest / len(cuts)))
        loudness = loudness * jnp.repeat(draws, shape[dim] // shards_of).reshape([-1 if axis == dim else 1 for axis in range(len(shape))])
    return loudness


def normal_values(key, shape, scale, most, cuts=(), kind=jnp.bfloat16):
    array = scale * jax.random.normal(key, shape, jnp.float32)
    if cuts:
        array = array * block_levels(key, shape, cuts, -0.22, 0.18)
    return jnp.clip(array, -most, most).astype(kind)


def setup_inputs(seed: int = 0) -> dict:
    streams_of = jax.random.split(jax.random.key(seed), 4)
    return {
        "inverse": normal_values(streams_of[0], (FRACS, M, M), M ** -0.5, 0.125, ((0, 32),)),
        "sources": normal_values(streams_of[1], (FRACS, M, R), 1.0, 6.0, ((0, 32),)),
        "slot_blocks": draw_slot_blocks(jax.random.fold_in(streams_of[3], 71), 0),
    }


penalty_weight = 0.5


def reference(inverse, sources, slot_blocks):
    nblocks = F_DEV * M // BLOCK
    cols = BLOCK * R
    slots = slot_blocks.shape[1]
    positions = jnp.arange(nblocks, dtype=jnp.int32)
    pick = (slot_blocks[:, :, None] == positions[None, None, :]).astype(jnp.float32)
    live = (slot_blocks >= 0).astype(jnp.float32)[:, :, None]

    def forward(columns):
        return lax.map(lambda pair: jnp.dot(pair[0], pair[1], preferred_element_type=jnp.float32), (inverse, columns))

    def backward(columns):
        return lax.map(lambda pair: jnp.dot(pair[0].T, pair[1], preferred_element_type=jnp.float32), (inverse, columns))

    def extract(field):
        shaped = field.reshape(DEVS, nblocks, cols)
        return jnp.einsum("dsb,dbc->dsc", pick, shaped, precision=lax.Precision.HIGHEST).astype(jnp.bfloat16)

    def collect(field):
        shaped = field.reshape(DEVS, nblocks, cols)
        return jnp.einsum("dsb,dbc->dsc", pick, shaped, precision=lax.Precision.HIGHEST)

    def embed(values):
        placed = jnp.einsum("dsb,dsc->dbc", pick, values, precision=lax.Precision.HIGHEST)
        return placed.reshape(FRACS, M, R).astype(jnp.bfloat16)

    def partners(moments):
        shaped = moments.reshape(N_GRP, N_MEM, slots, cols)
        near = shaped[:, :, :CAP]
        back = shaped[:, :, CAP:2 * CAP]
        cross = shaped[:, :, 2 * CAP:].reshape(N_GRP, N_MEM, N_MEM, CAPM, cols)
        ahead = jnp.roll(back, -1, axis=0)
        behind = jnp.roll(near, 1, axis=0)
        swapped = jnp.swapaxes(cross, 1, 2).reshape(N_GRP, N_MEM, N_MEM * CAPM, cols)
        return jnp.concatenate([ahead, behind, swapped], axis=2).reshape(DEVS, slots, cols)

    state = forward(sources)
    moments = extract(state)
    mismatch = live * (moments.astype(jnp.float32) - partners(moments).astype(jnp.float32))
    control = jnp.zeros((DEVS, slots, cols), jnp.float32)
    for step in range(ITERS):
        adj = backward(embed(mismatch))
        grad = collect(adj) + penalty_weight * control
        total_sq = jnp.sum(grad * grad)
        dstate = forward(embed(-grad))
        dmom = extract(dstate)
        dmis = live * (dmom.astype(jnp.float32) - partners(dmom).astype(jnp.float32))
        curv = 0.5 * jnp.sum(dmis * dmis)
        step_len = total_sq / (curv + penalty_weight * total_sq)
        control = control - step_len * grad
        state = state + step_len * dstate
        mismatch = mismatch + step_len * dmis
    return control, state.astype(jnp.bfloat16)
```

```python
import functools

import jax
import jax.numpy as jnp
from jax import lax
from jax.experimental import pallas as pl
from jax.experimental.pallas import tpu as pltpu
from jax.sharding import PartitionSpec as P

BLOCK = 128
CAP = 6
CAPM = 2
PENALTY = 0.5
F32 = jnp.float32
BF16 = jnp.bfloat16
MESH = pl.DeviceIdType.MESH


def kernel(
    sizes, table, inv_hbm, src_hbm, ctl_ref, out_ref,
    a, kmat, src, s0, v, vt, vm, g, h, d, mom, recv, red1, red2,
    load_sem, src_sem, send_sem, recv_sem, r1s, r1r, r2s, r2r,
):
    groups, members, tiles, near, slots = sizes
    width = s0.shape[2]
    nblocks, per = a.shape[:2]
    order = per * BLOCK
    live_slots = slots - CAPM
    rows = live_slots * BLOCK
    gi = lax.axis_index("grp")
    mi = lax.axis_index("mem")

    step_blocks = nblocks // tiles
    in_frac = per // step_blocks

    src_copy = pltpu.make_async_copy(src_hbm, src, src_sem)
    src_copy.start()

    def load(i, carry):
        f, r = lax.div(i, in_frac), lax.rem(i, in_frac)
        for j in range(per):
            pltpu.make_async_copy(
                inv_hbm.at[f, pl.ds(r * step_blocks, step_blocks), :, pl.ds(j * BLOCK, BLOCK)],
                a.at[pl.ds(i * step_blocks, step_blocks), j],
                load_sem.at[i],
            ).start()
        return carry

    lax.fori_loop(0, tiles, load, 0)

    barrier = pltpu.get_barrier_semaphore()
    for k in range(1, groups):
        pl.semaphore_signal(barrier, inc=1, device_id={"grp": lax.rem(gi + k, groups)}, device_id_type=MESH)
    for k in range(1, members):
        pl.semaphore_signal(barrier, inc=1, device_id={"mem": lax.rem(mi + k, members)}, device_id_type=MESH)

    def full_slot(c):
        j = (c - 2 * near) // CAPM
        k = (c - 2 * near) % CAPM
        return 2 * near + lax.rem(mi + 1 + j, members) * CAPM + k

    names = []
    for c in range(live_slots):
        names.append(table[c] if c < 2 * near else table[full_slot(c)])
    place = [jnp.maximum(t, 0) for t in names]
    frac = [lax.div(t, per) for t in place]
    column = [t - f * per for t, f in zip(place, frac)]
    alive = [(t >= 0).astype(F32) for t in names]

    def exchange(e):
        copies = []
        plan = [
            (0, near, near, {"grp": lax.rem(gi + 1, groups)}),
            (near, 0, near, {"grp": lax.rem(gi + groups - 1, groups)}),
        ]
        for j in range(members - 1):
            plan.append((
                2 * near + j * CAPM,
                2 * near + (members - 2 - j) * CAPM,
                CAPM,
                {"mem": lax.rem(mi + 1 + j, members)},
            ))
        for i, (at, to, count, device) in enumerate(plan):
            copies.append(pltpu.make_async_remote_copy(
                src_ref=mom.at[e, pl.ds(at, count)],
                dst_ref=recv.at[e, pl.ds(to, count)],
                send_sem=send_sem.at[e, i],
                recv_sem=recv_sem.at[e, i],
                device_id=device,
                device_id_type=MESH,
            ))
        return copies, [(to, count) for _, to, count, _ in plan]

    def take(moves, one, carry):
        copies, landed = moves
        for i in (*range(2, members + 1), 0, 1):
            copies[i].wait()
            carry = lax.fori_loop(landed[i][0], landed[i][0] + landed[i][1], one, carry)
        return carry

    src_copy.wait()

    def first(i, carry):
        whole = a.at[pl.ds(i * step_blocks, step_blocks)]
        pltpu.make_async_copy(whole, whole, load_sem.at[i]).wait()
        f = lax.div(i, in_frac)
        lhs = jnp.concatenate(
            [
                a[pl.ds(i * step_blocks, step_blocks), j].reshape(step_blocks * BLOCK, BLOCK)
                for j in range(per)
            ],
            axis=1,
        )
        prod = jnp.dot(lhs, src[f].reshape(order, width), preferred_element_type=F32)
        s0[pl.ds(i * step_blocks, step_blocks)] = prod.reshape(step_blocks, BLOCK, width)
        return carry

    lax.fori_loop(0, tiles, first, 0)

    for c in range(live_slots):
        x = s0[place[c]]
        mom[0, c] = (x * alive[c]).astype(BF16)
    pl.semaphore_wait(barrier, groups - 1 + members - 1)
    moves = exchange(0)
    for copy in (*moves[0][2:], *moves[0][:2]):
        copy.start()

    for r in range(live_slots):
        for c in range(live_slots):
            weight = (frac[r] == frac[c]).astype(F32) * alive[r] * alive[c]
            kmat[pl.ds(r * BLOCK, BLOCK), pl.ds(c * BLOCK, BLOCK)] = a[place[r], column[c]] * jnp.full(
                (BLOCK, BLOCK), weight, F32
            ).astype(BF16)

    def fold(x):
        return jnp.sum(x.reshape(BLOCK // 8, 8, width), axis=0)

    zero = jnp.zeros((8, width), F32)

    def to_vt(c, x):
        vt[:, pl.ds(pl.multiple_of(c * BLOCK, BLOCK), BLOCK)] = x.T.astype(BF16)

    def take0(c, carry):
        to_vt(c, mom[0, c].astype(F32) - recv[0, c].astype(F32))
        return carry

    take(moves, take0, 0)

    part = near
    parts_of = live_slots // part
    part_rows = part * BLOCK

    def adjoint(t, into):
        prod = jnp.dot(
            vt[...], kmat[:, pl.ds(pl.multiple_of(t * part_rows, part_rows), part_rows)],
            preferred_element_type=F32,
        ).T.reshape(part, BLOCK, width)
        into[pl.ds(t * part, part)] = prod
        v[pl.ds(t * part, part)] = prod.astype(BF16)

    def solve_and_send(e):
        moves = exchange(e)
        for t, ready in ((2, moves[0][2:]), (0, moves[0][:1]), (1, moves[0][1:2])):
            prod = jnp.dot(
                kmat[pl.ds(t * part_rows, part_rows), :],
                v[...].reshape(rows, width), preferred_element_type=F32,
            )
            mom[e, pl.ds(t * part, part)] = prod.reshape(part, BLOCK, width).astype(BF16)
            for copy in ready:
                copy.start()
        return moves

    def mask_fracs():
        for f in range(nblocks // per):
            for c in range(live_slots):
                weight = (frac[c] == f).astype(F32) * alive[c]
                vm[f, pl.ds(c * BLOCK, BLOCK)] = v[c] * jnp.full((BLOCK, width), weight, F32).astype(BF16)

    def solve_states(into, begin, end):
        def one(i, carry):
            f = lax.div(i, in_frac)
            lhs = jnp.concatenate(
                [
                    jnp.concatenate([a[step_blocks * i + b, column[c]] for b in range(step_blocks)], axis=0)
                    for c in range(live_slots)
                ],
                axis=1,
            )
            prod = jnp.dot(lhs, vm[f], preferred_element_type=F32)
            into[f, pl.ds(lax.rem(i, in_frac) * step_blocks, step_blocks)] = prod.reshape(
                step_blocks, BLOCK, width
            ).astype(BF16)
            return carry

        lax.fori_loop(begin, end, one, 0)

    def adj_g(t, carry):
        adjoint(t, g)
        return carry

    lax.fori_loop(0, parts_of, adj_g, 0)
    moves = solve_and_send(1)
    mask_fracs()
    solve_states(src, 0, tiles - 1)
    gg = lax.fori_loop(0, live_slots, lambda c, acc: acc + fold(g[c] * g[c]), zero)

    def take1(c, acc):
        x = recv[1, c].astype(F32) - mom[1, c].astype(F32)
        d[c] = x
        to_vt(c, x)
        return acc + fold(x * x)

    dd = take(moves, take1, zero)

    def adj_h(t, carry):
        adjoint(t, h)
        return carry

    lax.fori_loop(0, parts_of, adj_h, 0)
    moves = solve_and_send(2)
    solve_states(src, tiles - 1, tiles)
    mask_fracs()

    def norms(c, acc):
        gh, hh = acc
        return gh + fold(g[c] * h[c]), hh + fold(h[c] * h[c])

    gh, hh = lax.fori_loop(0, live_slots, norms, (zero, zero))
    solve_states(out_ref, 0, tiles - 3)

    def take2(c, acc):
        de, ee = acc
        x = recv[2, c].astype(F32) - mom[2, c].astype(F32)
        return de + fold(d[c] * x), ee + fold(x * x)

    de, ee = take(moves, take2, (zero, zero))

    row = lax.broadcasted_iota(jnp.int32, (8, 128), 0)
    pack = jnp.zeros((8, 128), F32)
    for q, part in enumerate((gg, gh, hh, dd, de, ee)):
        pack = jnp.where(row == q, jnp.sum(part), pack)
    red1[mi] = pack
    copies = [
        pltpu.make_async_remote_copy(
            src_ref=red1.at[mi], dst_ref=red1.at[mi],
            send_sem=r1s.at[k - 1], recv_sem=r1r.at[k - 1],
            device_id={"mem": lax.rem(mi + k, members)}, device_id_type=MESH,
        )
        for k in range(1, members)
    ]
    for copy in copies:
        copy.start()
    solve_states(out_ref, tiles - 3, tiles - 2)
    for copy in copies:
        copy.wait()
    red2[gi] = jnp.sum(red1[...], axis=0)
    copies = [
        pltpu.make_async_remote_copy(
            src_ref=red2.at[gi], dst_ref=red2.at[gi],
            send_sem=r2s.at[k - 1], recv_sem=r2r.at[k - 1],
            device_id={"grp": lax.rem(gi + k, groups)}, device_id_type=MESH,
        )
        for k in range(1, groups)
    ]
    for copy in copies:
        copy.start()
    solve_states(out_ref, tiles - 2, tiles)
    for copy in copies:
        copy.wait()
    total = jnp.sum(red2[...], axis=0)
    gg, gh, hh, dd, de, ee = [total[q : q + 1, :] for q in range(6)]
    step1 = gg / (0.5 * dd + PENALTY * gg)
    keep = 1.0 - PENALTY * step1
    sq2 = keep * keep * gg + 2.0 * keep * step1 * gh + step1 * step1 * hh
    dd2 = keep * keep * dd + 2.0 * keep * step1 * de + step1 * step1 * ee
    step2 = sq2 / (0.5 * dd2 + PENALTY * sq2)
    alpha = step1 + step2 * keep
    beta = step1 * step2
    alpha_w = jnp.concatenate([alpha] * (width // 128), axis=1)
    beta_w = jnp.concatenate([beta] * (width // 128), axis=1)

    parts = width // 128

    def put(slot, c):
        for q in range(parts):
            lanes = pl.ds(q * 128, 128)
            ctl_ref[slot, pl.ds(q, BLOCK, stride=parts), :] = -(
                alpha * g[c, :, lanes] + beta * h[c, :, lanes]
            )

    for c in range(live_slots):
        put(c if c < 2 * near else full_slot(c), c)
    for k in range(CAPM):
        ctl_ref[2 * near + mi * CAPM + k] = jnp.zeros((parts * BLOCK, 128), F32)

    def final(i, carry):
        f, r = lax.div(i, per), lax.rem(i, per)
        out_ref[f, r] = (
            s0[i] - alpha_w * src[f, r].astype(F32) - beta_w * out_ref[f, r].astype(F32)
        ).astype(BF16)
        return carry

    lax.fori_loop(0, nblocks, final, 0)


def per_device(inverse, sources, slot_blocks):
    members = lax.axis_size("mem")
    groups = lax.axis_size("grp")
    fracs, order, width = sources.shape
    slots = slot_blocks.shape[1]
    per = order // BLOCK
    nblocks = fracs * per
    tiles = nblocks // 4
    live = slots - CAPM
    rows = live * BLOCK
    vmem = pltpu.VMEM
    dma = pltpu.SemaphoreType.DMA
    control, states = pl.pallas_call(
        functools.partial(kernel, (groups, members, tiles, CAP, slots)),
        out_shape=(
            pltpu.VMEM((slots, BLOCK * width // 128, 128), F32),
            pltpu.VMEM((fracs, per, BLOCK, width), BF16),
        ),
        in_specs=[
            pl.BlockSpec(memory_space=pltpu.SMEM),
            pl.BlockSpec(memory_space=pl.ANY),
            pl.BlockSpec(memory_space=pl.ANY),
        ],
        out_specs=(pl.BlockSpec(memory_space=pltpu.VMEM), pl.BlockSpec(memory_space=pltpu.VMEM)),
        scratch_shapes=[
            vmem((nblocks, per, BLOCK, BLOCK), BF16),
            vmem((rows, rows), BF16),
            vmem((fracs, per, BLOCK, width), BF16),
            vmem((nblocks, BLOCK, width), F32),
            vmem((live, BLOCK, width), BF16),
            vmem((width, rows), BF16),
            vmem((fracs, rows, width), BF16),
            vmem((live, BLOCK, width), F32),
            vmem((live, BLOCK, width), F32),
            vmem((live, BLOCK, width), F32),
            vmem((3, live, BLOCK, width), BF16),
            vmem((3, live, BLOCK, width), BF16),
            vmem((members, 8, 128), F32),
            vmem((groups, 8, 128), F32),
            dma((tiles,)),
            dma,
            dma((3, members + 1)),
            dma((3, members + 1)),
            dma((members - 1,)),
            dma((members - 1,)),
            dma((groups - 1,)),
            dma((groups - 1,)),
        ],
        compiler_params=pltpu.CompilerParams(
            collective_id=0, has_side_effects=True, vmem_limit_bytes=61_000_000
        ),
    )(
        slot_blocks[0],
        inverse.reshape(fracs, per, BLOCK, order),
        sources.reshape(fracs, per, BLOCK, width),
    )
    return (control.reshape(1, slots, BLOCK * width), states.reshape(fracs, order, width))


def solution(mesh):
    in_specs = (
        P(("grp", "mem"), None, None),
        P(("grp", "mem"), None, None),
        P(("grp", "mem"), None),
    )
    out_specs = (P(("grp", "mem"), None, None), P(("grp", "mem"), None, None))
    return jax.shard_map(
        per_device, mesh=mesh, in_specs=in_specs, out_specs=out_specs, check_vma=False
    )
```

```python
import functools

import jax
import jax.numpy as jnp
from jax import lax
from jax.experimental import pallas as pl
from jax.experimental.pallas import tpu as pltpu
from jax.sharding import PartitionSpec as P

BLOCK = 128
CAP = 6
CAPM = 2
PENALTY = 0.5
HALVES = 2
F32 = jnp.float32
BF16 = jnp.bfloat16
MESH = pl.DeviceIdType.MESH


G1, G2, H1 = 3, 7, 4


def kernel(
    sizes, table, inv_hbm, src_hbm, g, out_h,
    a, kmat, kmat_t, out_g, s0, h, vt, vg, vm, mom, recv, red,
    load_sem, src_sem, send_sem, recv_sem, red_send, red_recv,
):
    groups, members, tiles, near, slots, halves = sizes
    width = s0.shape[2]
    half = width // halves
    nblocks, per = a.shape[:2]
    src = out_g
    order = per * BLOCK
    live_slots = slots - CAPM
    rows = live_slots * BLOCK
    gi = lax.axis_index("grp")
    mi = lax.axis_index("mem")

    step_blocks = nblocks // tiles
    in_frac = per // step_blocks

    src_copy = pltpu.make_async_copy(src_hbm, src, src_sem)
    src_copy.start()

    def load(i, carry):
        f, r = lax.div(i, in_frac), lax.rem(i, in_frac)
        for j in range(per):
            pltpu.make_async_copy(
                inv_hbm.at[f, pl.ds(r * step_blocks, step_blocks), :, pl.ds(j * BLOCK, BLOCK)],
                a.at[pl.ds(i * step_blocks, step_blocks), j],
                load_sem.at[i],
            ).start()
        return carry

    lax.fori_loop(0, tiles, load, 0)

    barrier = pltpu.get_barrier_semaphore()
    devices = groups * members
    me = gi * members + mi

    def peer(k):
        at = lax.rem(me + k, devices)
        return {"grp": lax.div(at, members), "mem": lax.rem(at, members)}

    def greet(k, carry):
        pl.semaphore_signal(barrier, inc=1, device_id=peer(k), device_id_type=MESH)
        return carry

    lax.fori_loop(1, devices, greet, 0)

    def full_slot(c):
        j = (c - 2 * near) // CAPM
        k = (c - 2 * near) % CAPM
        return 2 * near + lax.rem(mi + 1 + j, members) * CAPM + k

    names = []
    for c in range(live_slots):
        names.append(table[c] if c < 2 * near else table[full_slot(c)])
    place = [jnp.maximum(t, 0) for t in names]
    frac = [lax.div(t, per) for t in place]
    column = [t - f * per for t, f in zip(place, frac)]
    alive = [(t >= 0).astype(F32) for t in names]

    ahead = {"grp": lax.rem(gi + 1, groups)}
    behind = {"grp": lax.rem(gi + groups - 1, groups)}
    near_half = near // 2
    mem_half = CAPM // 2

    def offset(j):
        return 2 * near + j * CAPM

    def low(j):
        return lax.div(mi + 1 + j, members)

    def exchange(e, hf):
        if e < 2:
            plan = [(0, near, near, ahead), (near, 0, near, behind)]
            landed = [(near, near), (0, near)]
        else:
            plan = [(0, near, near_half, ahead), (near + near_half, near_half, near - near_half, behind)]
            landed = [(near, near_half), (near_half, near - near_half)]
        for j in range(members - 1):
            back = members - 2 - j
            device = {"mem": lax.rem(mi + 1 + j, members)}
            if e < 2:
                plan.append((offset(j), offset(back), CAPM, device))
                landed.append((offset(back), CAPM))
            else:
                at = low(j) * mem_half
                plan.append((offset(j) + at, offset(back) + at, mem_half, device))
                landed.append((offset(back) + (1 - low(back)) * mem_half, mem_half))
        copies = []
        for i, (at, to, count, device) in enumerate(plan):
            copies.append(pltpu.make_async_remote_copy(
                src_ref=mom.at[e % 2, hf, pl.ds(at, count)],
                dst_ref=recv.at[e % 2, hf, pl.ds(to, count)],
                send_sem=send_sem.at[e, hf, i],
                recv_sem=recv_sem.at[e, hf, i],
                device_id=device,
                device_id_type=MESH,
            ))
        return copies, landed

    def take(moves, one, carry):
        copies, landed = moves
        for i in (0, 1, *range(2, members + 1)):
            copies[i].wait()
            at, count = landed[i]
            for k in range(count):
                carry = one(at + k, carry)
        return carry

    src_copy.wait()

    def first(i, carry):
        whole = a.at[pl.ds(i * step_blocks, step_blocks)]
        pltpu.make_async_copy(whole, whole, load_sem.at[i]).wait()
        f = lax.div(i, in_frac)
        lhs = jnp.concatenate(
            [
                a[pl.ds(i * step_blocks, step_blocks), j].reshape(step_blocks * BLOCK, BLOCK)
                for j in range(per)
            ],
            axis=1,
        )
        prod = jnp.dot(lhs, src[f].reshape(order, width), preferred_element_type=F32)
        s0[pl.ds(i * step_blocks, step_blocks)] = prod.reshape(step_blocks, BLOCK, width)
        return carry

    lax.fori_loop(0, tiles, first, 0)

    def extract(hf, c):
        x = s0[place[c], :, pl.ds(hf * half, half)]
        mom[0, hf, c] = (x * alive[c]).T.astype(BF16)

    starts = []
    for hf in range(halves):
        moves = exchange(0, hf)
        for c in range(2 * near, live_slots):
            extract(hf, c)
        if hf == 0:
            pl.semaphore_wait(barrier, devices - 1)
        for copy in moves[0][2:]:
            copy.start()
        for c in range(2 * near):
            extract(hf, c)
        for copy in moves[0][:2]:
            copy.start()
        starts.append(moves)

    for r in range(live_slots):
        for c in range(live_slots):
            weight = (frac[r] == frac[c]).astype(F32) * alive[r] * alive[c]
            x = a[place[r], column[c]] * jnp.full((BLOCK, BLOCK), weight, F32).astype(BF16)
            kmat[pl.ds(r * BLOCK, BLOCK), pl.ds(c * BLOCK, BLOCK)] = x
            kmat_t[pl.ds(c * BLOCK, BLOCK), pl.ds(r * BLOCK, BLOCK)] = x.T

    def fold(x):
        return jnp.sum(x.reshape(x.shape[0] // 8, 8, x.shape[1]), axis=0)

    zero = jnp.zeros((8, 128), F32)
    small = jnp.zeros((8, BLOCK), F32)
    part = near
    parts_of = live_slots // part
    part_rows = part * BLOCK
    flipped = (((1,), (1,)), ((), ()))

    def adjoint(hf, into):
        for t in range(parts_of):
            prod = jnp.dot(
                vt[hf], kmat[:, pl.ds(t * part_rows, part_rows)], preferred_element_type=F32
            )
            vg[hf, :, pl.ds(t * part_rows, part_rows)] = prod.astype(BF16)
            for k in range(part):
                c = t * part + k
                x = prod[:, k * BLOCK : (k + 1) * BLOCK].T
                slot = c if c < 2 * near else full_slot(c)
                for q in range(half // 128):
                    into[slot, pl.ds(hf * (half // 128) + q, BLOCK, stride=width // 128), :] = x[
                        :, q * 128 : (q + 1) * 128
                    ]

    def solve_and_send(e, hf):
        moves = exchange(e, hf)
        copies = moves[0]
        for t, ready in ((2, copies[2:]), (0, copies[:1]), (1, copies[1:2])):
            prod = jnp.dot(
                vg[hf], kmat_t[:, pl.ds(t * part_rows, part_rows)], preferred_element_type=F32
            )
            for k in range(part):
                mom[e % 2, hf, t * part + k] = prod[:, k * BLOCK : (k + 1) * BLOCK].astype(BF16)
            for copy in ready:
                copy.start()
        return moves

    def mask_fracs(hf):
        for f in range(nblocks // per):
            for c in range(live_slots):
                weight = (frac[c] == f).astype(F32) * alive[c]
                cols = pl.ds(c * BLOCK, BLOCK)
                vm[f, pl.ds(hf * half, half), cols] = vg[hf, :, cols] * jnp.full(
                    (half, BLOCK), weight, F32
                ).astype(BF16)

    def solve_states(into, begin, end):
        def one(i, carry):
            f = lax.div(i, in_frac)
            lhs = jnp.concatenate(
                [
                    jnp.concatenate([a[step_blocks * i + b, column[c]] for b in range(step_blocks)], axis=0)
                    for c in range(live_slots)
                ],
                axis=1,
            )
            prod = lax.dot_general(lhs, vm[f], flipped, preferred_element_type=F32)
            into[f, pl.ds(lax.rem(i, in_frac) * step_blocks, step_blocks)] = prod.reshape(
                step_blocks, BLOCK, width
            ).astype(BF16)
            return carry

        if end > begin:
            lax.fori_loop(begin, end, one, 0)

    for k in range(CAPM):
        for into in (g, h):
            into[2 * near + mi * CAPM + k] = jnp.zeros(into.shape[1:], F32)

    second = []
    for hf in range(halves):

        def take0(c, carry):
            vt[hf, :, pl.ds(c * BLOCK, BLOCK)] = (mom[0, hf, c].astype(F32) - recv[0, hf, c].astype(F32)).astype(BF16)
            return carry

        take(starts[hf], take0, 0)
        adjoint(hf, g)
        second.append(solve_and_send(1, hf))
        mask_fracs(hf)

    solve_states(out_g, 0, G1)

    third = []
    dd = small
    for hf in range(halves):

        def take1(c, acc):
            x = recv[1, hf, c].astype(F32) - mom[1, hf, c].astype(F32)
            vt[hf, :, pl.ds(c * BLOCK, BLOCK)] = x.astype(BF16)
            return acc + fold(x * x)

        dd = take(second[hf], take1, dd)
        adjoint(hf, h)
        third.append(solve_and_send(2, hf))
        if hf == 0:
            solve_states(out_g, G1, G2)

    solve_states(out_g, G2, tiles)
    for hf in range(halves):
        mask_fracs(hf)
    solve_states(out_h, 0, H1)

    def norms(c, acc):
        gg, gh, hh = acc
        x, y = g[c], h[c]
        return gg + fold(x * x), gh + fold(x * y), hh + fold(y * y)

    gg, gh, hh = lax.fori_loop(0, slots, norms, (zero, zero, zero))

    kk = small
    for hf in range(halves):
        for c in range(live_slots):
            x = mom[0, hf, c].astype(F32)
            kk = kk + fold(x * x)
    cross = small
    for hf in range(halves):

        def take2(c, acc):
            return acc + fold(recv[0, hf, c].astype(F32) * mom[0, hf, c].astype(F32))

        cross = take(third[hf], take2, cross)

    lane = lax.broadcasted_iota(jnp.int32, (8, 128), 1)
    pack = jnp.zeros((8, 128), F32)
    for q, value in enumerate((gg, gh, hh, dd, kk - 2.0 * cross)):
        pack = jnp.where(lane == q, jnp.sum(value, axis=1, keepdims=True), pack)
    red[me] = jnp.sum(pack, axis=0, keepdims=True)

    def share(k):
        return pltpu.make_async_remote_copy(
            src_ref=red.at[me], dst_ref=red.at[me],
            send_sem=red_send.at[k - 1], recv_sem=red_recv.at[k - 1],
            device_id=peer(k), device_id_type=MESH,
        )

    def share_start(k, carry):
        share(k).start()
        return carry

    def share_wait(k, carry):
        share(k).wait()
        return carry

    lax.fori_loop(1, devices, share_start, 0)
    solve_states(out_h, H1, tiles)
    lax.fori_loop(1, devices, share_wait, 0)
    total = jnp.sum(red[...], axis=0)
    gg, gh, hh, dd, kk = [
        jnp.sum(jnp.where(lane[:1] == q, total, 0.0), axis=1, keepdims=True) for q in range(5)
    ]
    de, ee = -2.0 * hh, 2.0 * kk
    step1 = gg / (0.5 * dd + PENALTY * gg)
    keep = 1.0 - PENALTY * step1
    sq2 = keep * keep * gg + 2.0 * keep * step1 * gh + step1 * step1 * hh
    dd2 = jnp.maximum(keep * keep * dd + 2.0 * keep * step1 * de + step1 * step1 * ee, 0.0)
    step2 = sq2 / (0.5 * dd2 + PENALTY * sq2)
    alpha = step1 + step2 * keep
    beta = step1 * step2

    def controls(slot, carry):
        g[slot] = -(alpha * g[slot] + beta * h[slot])
        return carry

    lax.fori_loop(0, slots, controls, 0)

    def states(i, carry):
        f, r = lax.div(i, per), lax.rem(i, per)
        out_h[f, r] = (
            s0[i] - alpha * out_g[f, r].astype(F32) - beta * out_h[f, r].astype(F32)
        ).astype(BF16)
        return carry

    lax.fori_loop(0, nblocks, states, 0)


def per_device(inverse, sources, slot_blocks):
    members = lax.axis_size("mem")
    groups = lax.axis_size("grp")
    fracs, order, width = sources.shape
    slots = slot_blocks.shape[1]
    per = order // BLOCK
    nblocks = fracs * per
    tiles = nblocks // 4
    live = slots - CAPM
    rows = live * BLOCK
    halves = HALVES
    half = width // halves
    vmem = pltpu.VMEM
    dma = pltpu.SemaphoreType.DMA
    control, states = pl.pallas_call(
        functools.partial(kernel, (groups, members, tiles, CAP, slots, halves)),
        out_shape=(
            vmem((slots, BLOCK * width // 128, 128), F32),
            vmem((fracs, per, BLOCK, width), BF16),
        ),
        in_specs=[
            pl.BlockSpec(memory_space=pltpu.SMEM),
            pl.BlockSpec(memory_space=pl.ANY),
            pl.BlockSpec(memory_space=pl.ANY),
        ],
        out_specs=(pl.BlockSpec(memory_space=pltpu.VMEM),) * 2,
        scratch_shapes=[
            vmem((nblocks, per, BLOCK, BLOCK), BF16),
            vmem((rows, rows), BF16),
            vmem((rows, rows), BF16),
            vmem((fracs, per, BLOCK, width), BF16),
            vmem((nblocks, BLOCK, width), F32),
            vmem((slots, BLOCK * width // 128, 128), F32),
            vmem((halves, half, rows), BF16),
            vmem((halves, half, rows), BF16),
            vmem((fracs, width, rows), BF16),
            vmem((2, halves, live, half, BLOCK), BF16),
            vmem((2, halves, live, half, BLOCK), BF16),
            vmem((groups * members, 1, 128), F32),
            dma((tiles,)),
            dma,
            dma((3, halves, members + 1)),
            dma((3, halves, members + 1)),
            dma((groups * members - 1,)),
            dma((groups * members - 1,)),
        ],
        compiler_params=pltpu.CompilerParams(
            collective_id=0, has_side_effects=True, vmem_limit_bytes=61_500_000
        ),
    )(
        slot_blocks[0],
        inverse.reshape(fracs, per, BLOCK, order),
        sources.reshape(fracs, per, BLOCK, width),
    )
    return (control.reshape(1, slots, BLOCK * width), states.reshape(fracs, order, width))


def solution(mesh):
    in_specs = (
        P(("grp", "mem"), None, None),
        P(("grp", "mem"), None, None),
        P(("grp", "mem"), None),
    )
    out_specs = (P(("grp", "mem"), None, None), P(("grp", "mem"), None, None))
    return jax.shard_map(
        per_device, mesh=mesh, in_specs=in_specs, out_specs=out_specs, check_vma=False
    )
```

```python
import functools

import jax
import jax.numpy as jnp
from jax import lax
from jax.experimental import pallas as pl
from jax.experimental.pallas import tpu as pltpu
from jax.sharding import PartitionSpec as P

BLOCK = 128
CAP = 6
CAPM = 2
PENALTY = 0.5
HALVES = 2
F32 = jnp.float32
BF16 = jnp.bfloat16
MESH = pl.DeviceIdType.MESH


G1, G2, H1 = 2, 4, 2


def kernel(
    sizes, table, inv_hbm, src_hbm, g, out_h,
    a, kmat, kmat_t, out_g, s0, h, vt, vg, vm, mom, recv, red,
    load_sem, src_sem, send_sem, recv_sem, red_send, red_recv,
):
    groups, members, tiles, near, slots, halves = sizes
    width = s0.shape[2]
    half = width // halves
    nblocks, per = a.shape[:2]
    src = out_g
    order = per * BLOCK
    live_slots = slots - CAPM
    rows = live_slots * BLOCK
    gi = lax.axis_index("grp")
    mi = lax.axis_index("mem")

    step_blocks = nblocks // tiles
    in_frac = per // step_blocks

    src_copy = pltpu.make_async_copy(src_hbm, src, src_sem)
    src_copy.start()

    def load(i, carry):
        f, r = lax.div(i, in_frac), lax.rem(i, in_frac)
        for j in range(per):
            pltpu.make_async_copy(
                inv_hbm.at[f, pl.ds(r * step_blocks, step_blocks), :, pl.ds(j * BLOCK, BLOCK)],
                a.at[pl.ds(i * step_blocks, step_blocks), j],
                load_sem.at[i],
            ).start()
        return carry

    lax.fori_loop(0, tiles, load, 0)

    barrier = pltpu.get_barrier_semaphore()
    devices = groups * members
    me = gi * members + mi

    def peer(k):
        at = lax.rem(me + k, devices)
        return {"grp": lax.div(at, members), "mem": lax.rem(at, members)}

    def greet(k, carry):
        pl.semaphore_signal(barrier, inc=1, device_id=peer(k), device_id_type=MESH)
        return carry

    lax.fori_loop(1, devices, greet, 0)

    def full_slot(c):
        j = (c - 2 * near) // CAPM
        k = (c - 2 * near) % CAPM
        return 2 * near + lax.rem(mi + 1 + j, members) * CAPM + k

    names = []
    for c in range(live_slots):
        names.append(table[c] if c < 2 * near else table[full_slot(c)])
    place = [jnp.maximum(t, 0) for t in names]
    frac = [lax.div(t, per) for t in place]
    column = [t - f * per for t, f in zip(place, frac)]
    alive = [(t >= 0).astype(F32) for t in names]

    ahead = {"grp": lax.rem(gi + 1, groups)}
    behind = {"grp": lax.rem(gi + groups - 1, groups)}
    near_half = near // 2
    mem_half = CAPM // 2

    def offset(j):
        return 2 * near + j * CAPM

    def low(j):
        return lax.div(mi + 1 + j, members)

    def exchange(e, hf):
        if e < 2:
            plan = [(0, near, near, ahead), (near, 0, near, behind)]
            landed = [(near, near), (0, near)]
        else:
            plan = [(0, near, near_half, ahead), (near + near_half, near_half, near - near_half, behind)]
            landed = [(near, near_half), (near_half, near - near_half)]
        for j in range(members - 1):
            back = members - 2 - j
            device = {"mem": lax.rem(mi + 1 + j, members)}
            if e < 2:
                plan.append((offset(j), offset(back), CAPM, device))
                landed.append((offset(back), CAPM))
            else:
                at = low(j) * mem_half
                plan.append((offset(j) + at, offset(back) + at, mem_half, device))
                landed.append((offset(back) + (1 - low(back)) * mem_half, mem_half))
        copies = []
        for i, (at, to, count, device) in enumerate(plan):
            copies.append(pltpu.make_async_remote_copy(
                src_ref=mom.at[e % 2, hf, pl.ds(at, count)],
                dst_ref=recv.at[e % 2, hf, pl.ds(to, count)],
                send_sem=send_sem.at[e, hf, i],
                recv_sem=recv_sem.at[e, hf, i],
                device_id=device,
                device_id_type=MESH,
            ))
        return copies, landed

    def take(moves, one, carry):
        copies, landed = moves
        for i in (0, 1, *range(2, members + 1)):
            copies[i].wait()
            at, count = landed[i]
            for k in range(count):
                carry = one(at + k, carry)
        return carry

    src_copy.wait()

    def first(i, carry):
        whole = a.at[pl.ds(i * step_blocks, step_blocks)]
        pltpu.make_async_copy(whole, whole, load_sem.at[i]).wait()
        f = lax.div(i, in_frac)
        lhs = jnp.concatenate(
            [
                a[pl.ds(i * step_blocks, step_blocks), j].reshape(step_blocks * BLOCK, BLOCK)
                for j in range(per)
            ],
            axis=1,
        )
        prod = jnp.dot(lhs, src[f].reshape(order, width), preferred_element_type=F32)
        s0[pl.ds(i * step_blocks, step_blocks)] = prod.reshape(step_blocks, BLOCK, width)
        return carry

    lax.fori_loop(0, tiles, first, 0)

    def extract(hf, c):
        x = s0[place[c], :, pl.ds(hf * half, half)]
        mom[0, hf, c] = (x * alive[c]).T.astype(BF16)

    starts = []
    for hf in range(halves):
        moves = exchange(0, hf)
        for c in range(2 * near, live_slots):
            extract(hf, c)
        if hf == 0:
            pl.semaphore_wait(barrier, devices - 1)
        for copy in moves[0][2:]:
            copy.start()
        for c in range(2 * near):
            extract(hf, c)
        for copy in moves[0][:2]:
            copy.start()
        starts.append(moves)

    for r in range(live_slots):
        for c in range(live_slots):
            weight = (frac[r] == frac[c]).astype(F32) * alive[r] * alive[c]
            x = a[place[r], column[c]] * jnp.full((BLOCK, BLOCK), weight, F32).astype(BF16)
            kmat[pl.ds(r * BLOCK, BLOCK), pl.ds(c * BLOCK, BLOCK)] = x
            kmat_t[pl.ds(c * BLOCK, BLOCK), pl.ds(r * BLOCK, BLOCK)] = x.T

    def fold(x):
        return jnp.sum(x.reshape(x.shape[0] // 8, 8, x.shape[1]), axis=0)

    zero = jnp.zeros((8, 128), F32)
    small = jnp.zeros((8, BLOCK), F32)
    part = near
    parts_of = live_slots // part
    part_rows = part * BLOCK
    flipped = (((1,), (1,)), ((), ()))

    def adjoint(hf, into):
        for t in range(parts_of):
            prod = jnp.dot(
                vt[hf], kmat[:, pl.ds(t * part_rows, part_rows)], preferred_element_type=F32
            )
            vg[hf, :, pl.ds(t * part_rows, part_rows)] = prod.astype(BF16)
            for k in range(part):
                c = t * part + k
                x = prod[:, k * BLOCK : (k + 1) * BLOCK].T
                slot = c if c < 2 * near else full_slot(c)
                for q in range(half // 128):
                    into[slot, pl.ds(hf * (half // 128) + q, BLOCK, stride=width // 128), :] = x[
                        :, q * 128 : (q + 1) * 128
                    ]

    def solve_and_send(e, hf):
        moves = exchange(e, hf)
        copies = moves[0]
        for t, ready in ((2, copies[2:]), (0, copies[:1]), (1, copies[1:2])):
            prod = jnp.dot(
                vg[hf], kmat_t[:, pl.ds(t * part_rows, part_rows)], preferred_element_type=F32
            )
            for k in range(part):
                mom[e % 2, hf, t * part + k] = prod[:, k * BLOCK : (k + 1) * BLOCK].astype(BF16)
            for copy in ready:
                copy.start()
        return moves

    def mask_fracs(hf):
        for f in range(nblocks // per):
            for c in range(live_slots):
                weight = (frac[c] == f).astype(F32) * alive[c]
                cols = pl.ds(c * BLOCK, BLOCK)
                vm[f, pl.ds(hf * half, half), cols] = vg[hf, :, cols] * jnp.full(
                    (half, BLOCK), weight, F32
                ).astype(BF16)

    def solve_states(into, begin, end):
        def one(i, carry):
            f = lax.div(i, in_frac)
            lhs = jnp.concatenate(
                [
                    jnp.concatenate([a[step_blocks * i + b, column[c]] for b in range(step_blocks)], axis=0)
                    for c in range(live_slots)
                ],
                axis=1,
            )
            prod = lax.dot_general(lhs, vm[f], flipped, preferred_element_type=F32)
            into[f, pl.ds(lax.rem(i, in_frac) * step_blocks, step_blocks)] = prod.reshape(
                step_blocks, BLOCK, width
            ).astype(BF16)
            return carry

        if end > begin:
            lax.fori_loop(begin, end, one, 0)

    for k in range(CAPM):
        for into in (g, h):
            into[2 * near + mi * CAPM + k] = jnp.zeros(into.shape[1:], F32)

    second = []
    for hf in range(halves):

        def take0(c, carry):
            vt[hf, :, pl.ds(c * BLOCK, BLOCK)] = (mom[0, hf, c].astype(F32) - recv[0, hf, c].astype(F32)).astype(BF16)
            return carry

        take(starts[hf], take0, 0)
        adjoint(hf, g)
        second.append(solve_and_send(1, hf))
        mask_fracs(hf)

    solve_states(out_g, 0, G1)

    third = []
    dd = small
    for hf in range(halves):

        def take1(c, acc):
            x = recv[1, hf, c].astype(F32) - mom[1, hf, c].astype(F32)
            vt[hf, :, pl.ds(c * BLOCK, BLOCK)] = x.astype(BF16)
            return acc + fold(x * x)

        dd = take(second[hf], take1, dd)
        adjoint(hf, h)
        third.append(solve_and_send(2, hf))
        if hf == 0:
            solve_states(out_g, G1, G2)

    solve_states(out_g, G2, tiles)
    for hf in range(halves):
        mask_fracs(hf)
    solve_states(out_h, 0, H1)

    together = 4 if slots % 4 == 0 else 1

    def norms(i, acc):
        gg, gh, hh = acc
        for k in range(together):
            x, y = g[together * i + k], h[together * i + k]
            gg, gh, hh = gg + fold(x * x), gh + fold(x * y), hh + fold(y * y)
        return gg, gh, hh

    gg, gh, hh = lax.fori_loop(0, slots // together, norms, (zero, zero, zero))

    kk = small
    for hf in range(halves):
        for c in range(live_slots):
            x = mom[0, hf, c].astype(F32)
            kk = kk + fold(x * x)
    cross = small
    for hf in range(halves):

        def take2(c, acc):
            return acc + fold(recv[0, hf, c].astype(F32) * mom[0, hf, c].astype(F32))

        cross = take(third[hf], take2, cross)

    lane = lax.broadcasted_iota(jnp.int32, (8, 128), 1)
    pack = jnp.zeros((8, 128), F32)
    for q, value in enumerate((gg, gh, hh, dd, kk - 2.0 * cross)):
        pack = jnp.where(lane == q, jnp.sum(value, axis=1, keepdims=True), pack)
    red[me] = jnp.sum(pack, axis=0, keepdims=True)

    def share(k):
        return pltpu.make_async_remote_copy(
            src_ref=red.at[me], dst_ref=red.at[me],
            send_sem=red_send.at[k - 1], recv_sem=red_recv.at[k - 1],
            device_id=peer(k), device_id_type=MESH,
        )

    def share_start(k, carry):
        share(k).start()
        return carry

    def share_wait(k, carry):
        share(k).wait()
        return carry

    lax.fori_loop(1, devices, share_start, 0)
    solve_states(out_h, H1, tiles)
    lax.fori_loop(1, devices, share_wait, 0)
    total = jnp.sum(red[...], axis=0)
    gg, gh, hh, dd, kk = [
        jnp.sum(jnp.where(lane[:1] == q, total, 0.0), axis=1, keepdims=True) for q in range(5)
    ]
    de, ee = -2.0 * hh, 2.0 * kk
    step1 = gg / (0.5 * dd + PENALTY * gg)
    keep = 1.0 - PENALTY * step1
    sq2 = keep * keep * gg + 2.0 * keep * step1 * gh + step1 * step1 * hh
    dd2 = jnp.maximum(keep * keep * dd + 2.0 * keep * step1 * de + step1 * step1 * ee, 0.0)
    step2 = sq2 / (0.5 * dd2 + PENALTY * sq2)
    alpha = step1 + step2 * keep
    beta = step1 * step2

    def controls(i, carry):
        for k in range(together):
            slot = together * i + k
            g[slot] = -(alpha * g[slot] + beta * h[slot])
        return carry

    lax.fori_loop(0, slots // together, controls, 0)

    def states(r, carry):
        for f in range(nblocks // per):
            out_h[f, r] = (
                s0[f * per + r] - alpha * out_g[f, r].astype(F32) - beta * out_h[f, r].astype(F32)
            ).astype(BF16)
        return carry

    lax.fori_loop(0, per, states, 0)


def per_device(inverse, sources, slot_blocks):
    members = lax.axis_size("mem")
    groups = lax.axis_size("grp")
    fracs, order, width = sources.shape
    slots = slot_blocks.shape[1]
    per = order // BLOCK
    nblocks = fracs * per
    tiles = nblocks // 4
    live = slots - CAPM
    rows = live * BLOCK
    halves = HALVES
    half = width // halves
    vmem = pltpu.VMEM
    dma = pltpu.SemaphoreType.DMA
    control, states = pl.pallas_call(
        functools.partial(kernel, (groups, members, tiles, CAP, slots, halves)),
        out_shape=(
            vmem((slots, BLOCK * width // 128, 128), F32),
            vmem((fracs, per, BLOCK, width), BF16),
        ),
        in_specs=[
            pl.BlockSpec(memory_space=pltpu.SMEM),
            pl.BlockSpec(memory_space=pl.ANY),
            pl.BlockSpec(memory_space=pl.ANY),
        ],
        out_specs=(pl.BlockSpec(memory_space=pltpu.VMEM),) * 2,
        scratch_shapes=[
            vmem((nblocks, per, BLOCK, BLOCK), BF16),
            vmem((rows, rows), BF16),
            vmem((rows, rows), BF16),
            vmem((fracs, per, BLOCK, width), BF16),
            vmem((nblocks, BLOCK, width), F32),
            vmem((slots, BLOCK * width // 128, 128), F32),
            vmem((halves, half, rows), BF16),
            vmem((halves, half, rows), BF16),
            vmem((fracs, width, rows), BF16),
            vmem((2, halves, live, half, BLOCK), BF16),
            vmem((2, halves, live, half, BLOCK), BF16),
            vmem((groups * members, 1, 128), F32),
            dma((tiles,)),
            dma,
            dma((3, halves, members + 1)),
            dma((3, halves, members + 1)),
            dma((groups * members - 1,)),
            dma((groups * members - 1,)),
        ],
        compiler_params=pltpu.CompilerParams(
            collective_id=0, has_side_effects=True, vmem_limit_bytes=61_500_000
        ),
    )(
        slot_blocks[0],
        inverse.reshape(fracs, per, BLOCK, order),
        sources.reshape(fracs, per, BLOCK, width),
    )
    return (control.reshape(1, slots, BLOCK * width), states.reshape(fracs, order, width))


def solution(mesh):
    in_specs = (
        P(("grp", "mem"), None, None),
        P(("grp", "mem"), None, None),
        P(("grp", "mem"), None),
    )
    out_specs = (P(("grp", "mem"), None, None), P(("grp", "mem"), None, None))
    return jax.shard_map(
        per_device, mesh=mesh, in_specs=in_specs, out_specs=out_specs, check_vma=False
    )
```
